32 devices in a mesh: col: 4 (over y, core), row: 8 (over z, x).
Axes of the slice: x: 2, y: 2, z: 4, core: 2. Of those that a mesh axis runs over, the one named last changes fastest.
Arguments:
- column_table: float32 [32768, 512], P('row', 'col'), may hold values from -3 to 3
- bag_rows: int32 [256, 32], P('row'), may hold values from 0 to 32767
Outputs:
- row_table: float32 [8, 4096, 512], P(None, ('col', 'row'))
- pooled: float32 [256, 512], P('row', 'col')
The draws below stay inside these ranges and needn't reach their ends.
Inputs may be any that keep to these rules, and one draw needn't show every extreme that they name: `bag_rows`: row indices of the table; a few rows are named far more often than the rest.
All inputs are finite; a program needn't handle non-finite values.
Results may differ from the reference program's by a relative error of at most 0.000078.
Values sent between devices are 32-bit elements; how exact they have to be, the bound alone decides.
A program may use at most 64 MiB of HBM per device.

```python
import math
import jax
import jax.numpy as jnp
import numpy as np

E = 512
BAG_LEN = 32
ROWS = 32768
GROUPS = 8
BLOCK = 4096
BAGS = 256


def plant(drawn, own_key, low, top_value):
    place = [jax.random.randint(jax.random.fold_in(own_key, axis), (), 0, length) for axis, length in enumerate(drawn.shape)]
    longest = drawn.shape.index(max(drawn.shape))
    next_to = place[:longest] + [(place[longest] + 1) % drawn.shape[longest]] + place[longest + 1:]
    return drawn.at[tuple(place)].set(low).at[tuple(next_to)].set(top_value)


def steps_of(rng, shape, pieces, low, largest):
    gain = 1.0
    for position, shards_of in pieces:
        draws = jax.random.uniform(jax.random.fold_in(jax.random.fold_in(rng, 6), position), (shards_of,), jnp.float32, low / len(pieces), largest / len(pieces))
        gain = gain * jnp.repeat(jnp.exp(draws), shape[position] // shards_of).reshape((-1,) + (1,) * (len(shape) - 1 - position))
    return gain


def cumulative_ranks(count, lean):
    weights = [(1 << 20) // math.isqrt(grade ** lean) + 1 for grade in range(1, count + 1)]
    spread = 1 + sum(weights) // (1 << 30)
    return np.cumsum(np.array([max(1, weight // spread) for weight in weights]))


def ranked(own_key, dims, count, skew):
    table = cumulative_ranks(count, skew)
    lot = jax.random.randint(jax.random.fold_in(own_key, 1), dims, 0, int(table[count - 1]))
    standing = jnp.searchsorted(jnp.asarray(table, jnp.int32), lot, side="right")
    return jax.random.permutation(jax.random.fold_in(own_key, 2), count)[standing].astype(jnp.int32)


def bell_draw(rng, dims, scale, most, cuts=(), held_as=jnp.bfloat16):
    factor_of = steps_of(rng, dims, cuts, -0.22, 0.18) if cuts else 1.0
    values = jax.random.normal(rng, dims, jnp.float32) * scale * factor_of
    return jnp.minimum(jnp.maximum(values, -most), most).astype(held_as)


def setup_inputs(seed: int = 0) -> dict:
    key_list = jax.random.split(jax.random.key(seed), 3)
    column_table = bell_draw(key_list[0], (ROWS, E), 0.2, 3.0, ((0, 8), (1, 4)), jnp.float32)
    bag_rows = plant(ranked(key_list[1], (BAGS, BAG_LEN), ROWS, 2), jax.random.fold_in(key_list[1], 3), 0, ROWS - 1).astype(jnp.int32)
    return {"column_table": column_table, "bag_rows": bag_rows}


def reference(column_table, bag_rows):
    row_table = column_table.reshape(GROUPS, BLOCK, E)
    picked = jnp.take(column_table, bag_rows.reshape(-1), axis=0).reshape(BAGS, BAG_LEN, E)
    pooled = jnp.sum(picked.astype(jnp.float32), axis=1)
    return row_table, pooled
```

```python
import functools
import math

import jax
import jax.numpy as jnp
from jax import lax
from jax.experimental import pallas as pl
from jax.experimental.pallas import tpu as pltpu
from jax.sharding import PartitionSpec as P

MESH = pl.DeviceIdType.MESH
LANES = 128
SUBLANES = 8


def pooling(positions, table_rows):
    row_count = table_rows.shape[0]
    bag_count = positions.shape[0]
    block_rows = math.gcd(row_count, 512)
    turns = row_count // block_rows
    running = jnp.zeros((bag_count, table_rows.shape[1]), jnp.float32)
    tile_ids = jnp.arange(block_rows, dtype=jnp.int32)

    def advance(turn, carried):
        offset = turn * block_rows
        within = positions - offset
        matches = within[:, :, None] == tile_ids[None, None, :]
        counts = jnp.sum(matches.astype(jnp.float32), axis=1)
        table_block = lax.dynamic_slice_in_dim(table_rows, offset, block_rows, 0)
        return carried + jnp.dot(
            counts, table_block, precision=lax.Precision.HIGHEST, preferred_element_type=jnp.float32
        )

    return lax.fori_loop(0, turns, advance, running)


def general(column_table, bag_rows):
    row_groups = lax.axis_size("row")
    col_groups = lax.axis_size("col")
    block_len, col_width = column_table.shape
    full_width = col_width * col_groups
    span = block_len // (col_groups * row_groups)
    row_index = lax.axis_index("row")
    every_bag = lax.all_gather(bag_rows, "row", axis=0, tiled=True)
    sectioned = column_table.reshape(col_groups, row_groups, span, col_width)
    moved = lax.all_to_all(
        lax.all_to_all(sectioned, "col", split_axis=0, concat_axis=3, tiled=True),
        "row",
        split_axis=1,
        concat_axis=0,
        tiled=True,
    )
    row_table = moved.reshape(row_groups, span, full_width)
    first_row = row_index * block_len
    shifted = every_bag - first_row
    inside = (shifted >= 0) & (shifted < block_len)
    positions = jnp.where(inside, shifted, -1)
    pooled = lax.psum_scatter(
        pooling(positions, column_table), "row", scatter_dimension=0, tiled=True
    )
    return (row_table, pooled)


def flipped(index, mask, count):
    result, bit = 0, 1
    while bit < count:
        digit = lax.rem(lax.div(index, bit), 2)
        result = result + (1 - digit if mask & bit else digit) * bit
        bit *= 2
    return result


def kernel(
    row_groups, col_groups,
    table_ref, bags_ref, out_ref, pooled_ref,
    table_v, packed, gathered, counts, partial, arrived,
    load_sem, own_sem, send_sem, recv_sem, bag_send, bag_recv, sum_send, sum_recv,
):
    rows, cols = row_groups, col_groups
    r, c = lax.axis_index("row"), lax.axis_index("col")
    block_len, width = table_ref.shape
    span = block_len // (rows * cols)
    own_bags, bag_len = bags_ref.shape
    per_vreg = LANES // bag_len
    flat = c * rows + r

    load = pltpu.make_async_copy(table_ref, table_v, load_sem)
    load.start()
    lane0 = pl.multiple_of(c * width, width)
    own = pltpu.make_async_copy(
        table_ref.at[pl.ds(flat * span, span), :],
        out_ref.at[r, :, pl.ds(lane0, width)],
        own_sem,
    )
    own.start()

    tile_bags = own_bags // per_vreg
    packed[...] = jnp.concatenate(
        [bags_ref[q * tile_bags:(q + 1) * tile_bags, :] for q in range(per_vreg)], axis=1
    )
    gathered[r] = packed[...]

    masks = [(mr, mc) for mr in range(rows) for mc in range(cols) if (mr, mc) != (0, 0)]
    far = [m for m in masks if m[0] >= rows // 2]
    near = [m for m in masks if m[0] < rows // 2]
    far = sorted(far, key=lambda m: -m[0])
    near = sorted(near, key=lambda m: -m[0])
    order = ORDER(far, near)

    def peer(mr, mc):
        return flipped(r, mr, rows), flipped(c, mc, cols)

    barrier = pltpu.get_barrier_semaphore()
    for mr, mc in order:
        pr, pc = peer(mr, mc)
        pl.semaphore_signal(barrier, inc=1, device_id=(pc, pr), device_id_type=MESH)
    load.wait()
    pl.semaphore_wait(barrier, len(order))

    bag_copies = []
    for mr in range(1, rows):
        pr, _ = peer(mr, 0)
        copy = pltpu.make_async_remote_copy(
            src_ref=packed, dst_ref=gathered.at[r],
            send_sem=bag_send.at[mr], recv_sem=bag_recv.at[mr],
            device_id=(c, pr), device_id_type=MESH,
        )
        copy.start()
        bag_copies.append(copy)

    copies = []
    for i, (mr, mc) in enumerate(order):
        pr, pc = peer(mr, mc)
        copy = pltpu.make_async_remote_copy(
            src_ref=table_v.at[pl.ds((pc * rows + pr) * span, span), :],
            dst_ref=out_ref.at[r, :, pl.ds(lane0, width)],
            send_sem=send_sem.at[i], recv_sem=recv_sem.at[i],
            device_id=(pc, pr), device_id_type=MESH,
        )
        copy.start()
        copies.append((pr, pc, copy))

    for copy in bag_copies:
        copy.wait()

    chunk = math.gcd(block_len, 16 * LANES)
    lanes = lax.broadcasted_iota(jnp.int32, (tile_bags, chunk), 1)

    def count(group, _):
        shifted = gathered[group] - r * block_len
        for q in range(per_vreg):
            at = group * own_bags + q * tile_bags
            for part in range(block_len // chunk):
                here = shifted - part * chunk
                total = jnp.zeros((tile_bags, chunk), jnp.float32)
                for l in range(bag_len):
                    lane = q * bag_len + l
                    total += jnp.where(here[:, lane:lane + 1] == lanes, 1.0, 0.0)
                counts[pl.ds(at, tile_bags), part * chunk:(part + 1) * chunk] = total
        return 0

    lax.fori_loop(0, rows, count, 0)

    depth = math.gcd(block_len, 512)
    partial[...] = jnp.zeros_like(partial)

    def multiply(turn, _):
        at = pl.multiple_of(turn * depth, depth)
        block = table_v[pl.ds(at, depth), :]
        times = counts[:, pl.ds(at, depth)].astype(jnp.bfloat16)
        high = block.astype(jnp.bfloat16)
        rest = block - high.astype(jnp.float32)
        middle = rest.astype(jnp.bfloat16)
        low = (rest - middle.astype(jnp.float32)).astype(jnp.bfloat16)
        dot = functools.partial(jnp.dot, preferred_element_type=jnp.float32)
        both = dot(times, jnp.concatenate([high, middle], axis=1))
        step = (dot(times, low) + both[:, width:]) + both[:, :width]
        partial[...] += step.reshape(partial.shape)
        return 0

    lax.fori_loop(0, block_len // depth, multiply, 0)

    sum_copies = []
    for mr in range(1, rows):
        pr, _ = peer(mr, 0)
        copy = pltpu.make_async_remote_copy(
            src_ref=partial.at[pr], dst_ref=arrived.at[mr],
            send_sem=sum_send.at[mr], recv_sem=sum_recv.at[mr],
            device_id=(c, pr), device_id_type=MESH,
        )
        copy.start()
        sum_copies.append(copy)

    own.wait()
    for copy in sum_copies:
        copy.wait()
    total = partial[r]
    for mr in range(1, rows):
        total += arrived[mr]
    pooled_ref[...] = total
    for pr, pc, copy in copies:
        copy.wait()


def ORDER(far, near):
    return far + near


def per_device(column_table, bag_rows):
    rows, cols = lax.axis_size("row"), lax.axis_size("col")
    block_len, width = column_table.shape
    own_bags, bag_len = bag_rows.shape
    span = block_len // (rows * cols)
    fits = (
        width % LANES == 0 and LANES % bag_len == 0 and own_bags * bag_len == SUBLANES * LANES
        and span % SUBLANES == 0 and block_len % LANES == 0
        and rows & (rows - 1) == 0 and cols & (cols - 1) == 0
    )
    if not fits:
        return general(column_table, bag_rows)
    bags = own_bags * rows
    peers = rows * cols - 1
    dma = pltpu.SemaphoreType.DMA
    return pl.pallas_call(
        functools.partial(kernel, rows, cols),
        out_shape=(
            jax.ShapeDtypeStruct((rows, span, width * cols), jnp.float32),
            jax.ShapeDtypeStruct((own_bags, width), jnp.float32),
        ),
        in_specs=[pl.BlockSpec(memory_space=pltpu.HBM), pl.BlockSpec(memory_space=pltpu.VMEM)],
        out_specs=(pl.BlockSpec(memory_space=pltpu.VMEM), pl.BlockSpec(memory_space=pltpu.VMEM)),
        scratch_shapes=[
            pltpu.VMEM((block_len, width), jnp.float32),
            pltpu.VMEM((SUBLANES, LANES), jnp.int32),
            pltpu.VMEM((rows, SUBLANES, LANES), jnp.int32),
            pltpu.VMEM((bags, block_len), jnp.float32),
            pltpu.VMEM((rows, own_bags, width), jnp.float32),
            pltpu.VMEM((rows, own_bags, width), jnp.float32),
            dma, dma, dma((peers,)), dma((peers,)),
            dma((rows,)), dma((rows,)), dma((rows,)), dma((rows,)),
        ],
        compiler_params=pltpu.CompilerParams(
            collective_id=0, has_side_effects=True, vmem_limit_bytes=32 * 1024 * 1024
        ),
    )(column_table, bag_rows)


def solution(mesh):
    return jax.shard_map(
        per_device,
        mesh=mesh,
        in_specs=(P("row", "col"), P("row", None)),
        out_specs=(P(None, ("col", "row"), None), P("row", "col")),
        check_vma=False,
    )
```

```python
import functools
import math

import jax
import jax.numpy as jnp
from jax import lax
from jax.experimental import pallas as pl
from jax.experimental.pallas import tpu as pltpu
from jax.sharding import PartitionSpec as P

MESH = pl.DeviceIdType.MESH
LANES = 128
SUBLANES = 8


def pooling(positions, table_rows):
    row_count = table_rows.shape[0]
    bag_count = positions.shape[0]
    block_rows = math.gcd(row_count, 512)
    turns = row_count // block_rows
    running = jnp.zeros((bag_count, table_rows.shape[1]), jnp.float32)
    tile_ids = jnp.arange(block_rows, dtype=jnp.int32)

    def advance(turn, carried):
        offset = turn * block_rows
        within = positions - offset
        matches = within[:, :, None] == tile_ids[None, None, :]
        counts = jnp.sum(matches.astype(jnp.float32), axis=1)
        table_block = lax.dynamic_slice_in_dim(table_rows, offset, block_rows, 0)
        return carried + jnp.dot(
            counts, table_block, precision=lax.Precision.HIGHEST, preferred_element_type=jnp.float32
        )

    return lax.fori_loop(0, turns, advance, running)


def general(column_table, bag_rows):
    row_groups = lax.axis_size("row")
    col_groups = lax.axis_size("col")
    block_len, col_width = column_table.shape
    full_width = col_width * col_groups
    span = block_len // (col_groups * row_groups)
    row_index = lax.axis_index("row")
    every_bag = lax.all_gather(bag_rows, "row", axis=0, tiled=True)
    sectioned = column_table.reshape(col_groups, row_groups, span, col_width)
    moved = lax.all_to_all(
        lax.all_to_all(sectioned, "col", split_axis=0, concat_axis=3, tiled=True),
        "row",
        split_axis=1,
        concat_axis=0,
        tiled=True,
    )
    row_table = moved.reshape(row_groups, span, full_width)
    first_row = row_index * block_len
    shifted = every_bag - first_row
    inside = (shifted >= 0) & (shifted < block_len)
    positions = jnp.where(inside, shifted, -1)
    pooled = lax.psum_scatter(
        pooling(positions, column_table), "row", scatter_dimension=0, tiled=True
    )
    return (row_table, pooled)


def flipped(index, mask, count):
    result, bit = 0, 1
    while bit < count:
        digit = lax.rem(lax.div(index, bit), 2)
        result = result + (1 - digit if mask & bit else digit) * bit
        bit *= 2
    return result


def kernel(
    row_groups, col_groups,
    table_ref, bags_ref, out_ref, pooled_ref,
    table_v, bags_v, packed, gathered, counts, partial, arrived, halves, crossed,
    load_sem, bag_sem, own_sem, send_sem, recv_sem, bag_send, bag_recv, sum_send, sum_recv, cross_send, cross_recv,
):
    rows, cols = row_groups, col_groups
    r, c = lax.axis_index("row"), lax.axis_index("col")
    block_len, width = table_ref.shape
    span = block_len // (rows * cols)
    own_bags, bag_len = bags_ref.shape
    per_vreg = LANES // bag_len
    flat = c * rows + r

    bag_load = pltpu.make_async_copy(bags_ref, bags_v, bag_sem)
    bag_load.start()
    load = pltpu.make_async_copy(table_ref, table_v, load_sem)
    load.start()
    lane0 = pl.multiple_of(c * width, width)
    own = pltpu.make_async_copy(
        table_ref.at[pl.ds(flat * span, span), :],
        out_ref.at[r, :, pl.ds(lane0, width)],
        own_sem,
    )
    own.start()

    masks = [(mr, mc) for mr in range(rows) for mc in range(cols) if (mr, mc) != (0, 0)]
    half = rows // 2
    far = [m for m in masks if m[0] >= half]
    near = sorted((m for m in masks if m[0] < half), key=lambda m: -m[0])
    order = [m for pair in zip(far, near + [None]) for m in pair if m]
    cuts = [len(order) * n // 31 for n in CUTS]

    def peer(mr, mc):
        return flipped(r, mr, rows), flipped(c, mc, cols)

    barrier = pltpu.get_barrier_semaphore()
    for mr, mc in order:
        pr, pc = peer(mr, mc)
        pl.semaphore_signal(barrier, inc=1, device_id=(pc, pr), device_id_type=MESH)
    bag_load.wait()
    tile_bags = own_bags // per_vreg
    packed[...] = jnp.concatenate(
        [bags_v[q * tile_bags:(q + 1) * tile_bags, :] for q in range(per_vreg)], axis=1
    )
    gathered[r] = packed[...]
    load.wait()
    pl.semaphore_wait(barrier, len(order))

    bag_copies = []
    for mr in range(1, rows):
        pr, _ = peer(mr, 0)
        copy = pltpu.make_async_remote_copy(
            src_ref=packed, dst_ref=gathered.at[r],
            send_sem=bag_send.at[mr], recv_sem=bag_recv.at[mr],
            device_id=(c, pr), device_id_type=MESH,
        )
        copy.start()
        bag_copies.append(copy)

    copies = []

    def send(first, last):
        for i in range(first, last):
            mr, mc = order[i]
            pr, pc = peer(mr, mc)
            send_one(i, pr, pc)

    def send_one(i, pr, pc):
        copy = pltpu.make_async_remote_copy(
            src_ref=table_v.at[pl.ds((pc * rows + pr) * span, span), :],
            dst_ref=out_ref.at[r, :, pl.ds(lane0, width)],
            send_sem=send_sem.at[i], recv_sem=recv_sem.at[i],
            device_id=(pc, pr), device_id_type=MESH,
        )
        copy.start()
        copies.append(copy)

    send(0, cuts[0])

    for copy in bag_copies:
        copy.wait()

    chunk = math.gcd(block_len, 16 * LANES)
    lanes = lax.broadcasted_iota(jnp.int32, (tile_bags, chunk), 1)

    def count(group, _):
        shifted = gathered[group] - r * block_len
        for q in range(per_vreg):
            at = group * own_bags + q * tile_bags
            for part in range(block_len // chunk):
                here = shifted - part * chunk
                total = jnp.zeros((tile_bags, chunk), jnp.float32)
                for l in range(bag_len):
                    lane = q * bag_len + l
                    total += jnp.where(here[:, lane:lane + 1] == lanes, 1.0, 0.0)
                counts[pl.ds(at, tile_bags), part * chunk:(part + 1) * chunk] = total
        return 0

    lax.fori_loop(0, rows, count, 0)
    send(cuts[0], cuts[1])

    depth = math.gcd(block_len, 512)
    partial[...] = jnp.zeros_like(partial)

    def multiply(turn, _):
        at = pl.multiple_of(turn * depth, depth)
        block = table_v[pl.ds(at, depth), :]
        times = counts[:, pl.ds(at, depth)].astype(jnp.bfloat16)
        high = block.astype(jnp.bfloat16)
        rest = block - high.astype(jnp.float32)
        middle = rest.astype(jnp.bfloat16)
        low = (rest - middle.astype(jnp.float32)).astype(jnp.bfloat16)
        dot = functools.partial(jnp.dot, preferred_element_type=jnp.float32)
        both = dot(times, jnp.concatenate([high, middle], axis=1))
        step = (dot(times, low) + both[:, width:]) + both[:, :width]
        partial[...] += step.reshape(partial.shape)
        return 0

    lax.fori_loop(0, block_len // depth, multiply, 0)

    low, high = lax.rem(r, half), lax.div(r, half)
    sum_copies = []
    for mr in range(1, half):
        pr, _ = peer(mr, 0)
        copy = pltpu.make_async_remote_copy(
            src_ref=partial.at[:, lax.rem(pr, half)], dst_ref=arrived.at[mr],
            send_sem=sum_send.at[mr], recv_sem=sum_recv.at[mr],
            device_id=(c, pr), device_id_type=MESH,
        )
        copy.start()
        sum_copies.append(copy)
    send(cuts[1], cuts[2])

    for copy in sum_copies:
        copy.wait()
    total = partial[:, low]
    for mr in range(1, half):
        total += arrived[mr]
    halves[...] = total
    own.wait()
    other, _ = peer(half, 0)
    across = pltpu.make_async_remote_copy(
        src_ref=halves.at[1 - high], dst_ref=crossed,
        send_sem=cross_send, recv_sem=cross_recv,
        device_id=(c, other), device_id_type=MESH,
    )
    across.start()
    send(cuts[2], len(order))
    across.wait()
    pooled_ref[...] = halves[high] + crossed[...]
    for copy in copies:
        copy.wait()


CUTS = (16, 21, 26)


def per_device(column_table, bag_rows):
    rows, cols = lax.axis_size("row"), lax.axis_size("col")
    block_len, width = column_table.shape
    own_bags, bag_len = bag_rows.shape
    span = block_len // (rows * cols)
    fits = (
        width % LANES == 0 and LANES % bag_len == 0 and own_bags * bag_len == SUBLANES * LANES
        and span % SUBLANES == 0 and block_len % LANES == 0
        and rows > 1 and rows & (rows - 1) == 0 and cols & (cols - 1) == 0
    )
    if not fits:
        return general(column_table, bag_rows)
    bags = own_bags * rows
    peers = rows * cols - 1
    half = rows // 2
    dma = pltpu.SemaphoreType.DMA
    return pl.pallas_call(
        functools.partial(kernel, rows, cols),
        out_shape=(
            jax.ShapeDtypeStruct((rows, span, width * cols), jnp.float32),
            jax.ShapeDtypeStruct((own_bags, width), jnp.float32),
        ),
        in_specs=[pl.BlockSpec(memory_space=pltpu.HBM), pl.BlockSpec(memory_space=pltpu.HBM)],
        out_specs=(pl.BlockSpec(memory_space=pltpu.VMEM), pl.BlockSpec(memory_space=pltpu.VMEM)),
        scratch_shapes=[
            pltpu.VMEM((block_len, width), jnp.float32),
            pltpu.VMEM((own_bags, bag_len), jnp.int32),
            pltpu.VMEM((SUBLANES, LANES), jnp.int32),
            pltpu.VMEM((rows, SUBLANES, LANES), jnp.int32),
            pltpu.VMEM((bags, block_len), jnp.float32),
            pltpu.VMEM((2, half, own_bags, width), jnp.float32),
            pltpu.VMEM((half, 2, own_bags, width), jnp.float32),
            pltpu.VMEM((2, own_bags, width), jnp.float32),
            pltpu.VMEM((own_bags, width), jnp.float32),
            dma, dma, dma, dma((peers,)), dma((peers,)),
            dma((rows,)), dma((rows,)), dma((half,)), dma((half,)), dma, dma,
        ],
        compiler_params=pltpu.CompilerParams(
            collective_id=0, has_side_effects=True, vmem_limit_bytes=32 * 1024 * 1024
        ),
    )(
        pltpu.with_memory_space_constraint(column_table, pltpu.HBM),
        pltpu.with_memory_space_constraint(bag_rows, pltpu.HBM),
    )


def solution(mesh):
    return jax.shard_map(
        per_device,
        mesh=mesh,
        in_specs=(P("row", "col"), P("row", None)),
        out_specs=(P(None, ("col", "row"), None), P("row", "col")),
        check_vma=False,
    )
```

```python
import functools
import math

import jax
import jax.numpy as jnp
from jax import lax
from jax.experimental import pallas as pl
from jax.experimental.pallas import tpu as pltpu
from jax.sharding import PartitionSpec as P

MESH = pl.DeviceIdType.MESH
LANES = 128
SUBLANES = 8


def pooling(positions, table_rows):
    row_count = table_rows.shape[0]
    bag_count = positions.shape[0]
    block_rows = math.gcd(row_count, 512)
    turns = row_count // block_rows
    running = jnp.zeros((bag_count, table_rows.shape[1]), jnp.float32)
    tile_ids = jnp.arange(block_rows, dtype=jnp.int32)

    def advance(turn, carried):
        offset = turn * block_rows
        within = positions - offset
        matches = within[:, :, None] == tile_ids[None, None, :]
        counts = jnp.sum(matches.astype(jnp.float32), axis=1)
        table_block = lax.dynamic_slice_in_dim(table_rows, offset, block_rows, 0)
        return carried + jnp.dot(
            counts, table_block, precision=lax.Precision.HIGHEST, preferred_element_type=jnp.float32
        )

    return lax.fori_loop(0, turns, advance, running)


def general(column_table, bag_rows):
    row_groups = lax.axis_size("row")
    col_groups = lax.axis_size("col")
    block_len, col_width = column_table.shape
    full_width = col_width * col_groups
    span = block_len // (col_groups * row_groups)
    row_index = lax.axis_index("row")
    every_bag = lax.all_gather(bag_rows, "row", axis=0, tiled=True)
    sectioned = column_table.reshape(col_groups, row_groups, span, col_width)
    moved = lax.all_to_all(
        lax.all_to_all(sectioned, "col", split_axis=0, concat_axis=3, tiled=True),
        "row",
        split_axis=1,
        concat_axis=0,
        tiled=True,
    )
    row_table = moved.reshape(row_groups, span, full_width)
    first_row = row_index * block_len
    shifted = every_bag - first_row
    inside = (shifted >= 0) & (shifted < block_len)
    positions = jnp.where(inside, shifted, -1)
    pooled = lax.psum_scatter(
        pooling(positions, column_table), "row", scatter_dimension=0, tiled=True
    )
    return (row_table, pooled)


def flipped(index, mask, count):
    result, bit = 0, 1
    while bit < count:
        digit = lax.rem(lax.div(index, bit), 2)
        result = result + (1 - digit if mask & bit else digit) * bit
        bit *= 2
    return result


def kernel(
    row_groups, col_groups,
    table_ref, bags_ref, out_ref, pooled_ref,
    table_v, bags_v, packed, gathered, counts, partial, arrived, halves, crossed,
    load_sem, bag_sem, own_sem, send_sem, recv_sem, bag_send, bag_recv, sum_send, sum_recv, cross_send, cross_recv,
):
    rows, cols = row_groups, col_groups
    r, c = lax.axis_index("row"), lax.axis_index("col")
    block_len, width = table_ref.shape
    span = block_len // (rows * cols)
    own_bags, bag_len = bags_ref.shape
    per_vreg = LANES // bag_len
    flat = c * rows + r

    bag_load = pltpu.make_async_copy(bags_ref, bags_v, bag_sem)
    bag_load.start()
    load = pltpu.make_async_copy(table_ref, table_v, load_sem)
    load.start()
    own = pltpu.make_async_copy(
        table_ref.at[pl.ds(flat * span, span), :],
        out_ref.at[r, c],
        own_sem,
    )
    own.start()

    masks = [(mr, mc) for mr in range(rows) for mc in range(cols) if (mr, mc) != (0, 0)]
    half = rows // 2
    far = [m for m in masks if m[0] >= half]
    near = sorted((m for m in masks if m[0] < half), key=lambda m: -m[0])
    far = sorted(far, key=lambda m: (m[0] >= half + half // 2, m[1], m[0]))
    order = [m for pair in zip(far, near + [None]) for m in pair if m]
    cuts = [len(order) * n // 31 for n in CUTS]

    def peer(mr, mc):
        return flipped(r, mr, rows), flipped(c, mc, cols)

    barrier = pltpu.get_barrier_semaphore()
    for mr, mc in sorted(order, reverse=True):
        pr, pc = peer(mr, mc)
        pl.semaphore_signal(barrier, inc=1, device_id=(pc, pr), device_id_type=MESH)
    bag_load.wait()
    tile_bags = own_bags // per_vreg
    packed[...] = jnp.concatenate(
        [bags_v[q * tile_bags:(q + 1) * tile_bags, :] for q in range(per_vreg)], axis=1
    )
    gathered[r] = packed[...]
    load.wait()
    pl.semaphore_wait(barrier, len(order))

    bag_copies = []
    for mr in range(1, rows):
        pr, _ = peer(mr, 0)
        copy = pltpu.make_async_remote_copy(
            src_ref=packed, dst_ref=gathered.at[r],
            send_sem=bag_send.at[mr], recv_sem=bag_recv.at[mr],
            device_id=(c, pr), device_id_type=MESH,
        )
        copy.start()
        bag_copies.append(copy)

    copies = []

    def send(first, last):
        for i in range(first, last):
            mr, mc = order[i]
            pr, pc = peer(mr, mc)
            send_one(i, pr, pc)

    def send_one(i, pr, pc):
        copy = pltpu.make_async_remote_copy(
            src_ref=table_v.at[pl.ds((pc * rows + pr) * span, span), :],
            dst_ref=out_ref.at[r, c],
            send_sem=send_sem.at[i], recv_sem=recv_sem.at[i],
            device_id=(pc, pr), device_id_type=MESH,
        )
        copy.start()
        copies.append(copy)

    send(0, cuts[0])

    for copy in bag_copies:
        copy.wait()

    chunk = math.gcd(block_len, 16 * LANES)
    lanes = lax.broadcasted_iota(jnp.int32, (tile_bags, chunk), 1)

    def count(group, _):
        shifted = gathered[group] - r * block_len
        for q in range(per_vreg):
            at = group * own_bags + q * tile_bags
            for part in range(block_len // chunk):
                here = shifted - part * chunk
                total = jnp.zeros((tile_bags, chunk), jnp.float32)
                for l in range(bag_len):
                    lane = q * bag_len + l
                    total += jnp.where(here[:, lane:lane + 1] == lanes, 1.0, 0.0)
                counts[pl.ds(at, tile_bags), part * chunk:(part + 1) * chunk] = total
        return 0

    lax.fori_loop(0, rows, count, 0)
    send(cuts[0], cuts[1])

    depth = math.gcd(block_len, 512)
    partial[...] = jnp.zeros_like(partial)

    def multiply(turn, _):
        at = pl.multiple_of(turn * depth, depth)
        block = table_v[pl.ds(at, depth), :]
        times = counts[:, pl.ds(at, depth)].astype(jnp.bfloat16)
        high = block.astype(jnp.bfloat16)
        rest = block - high.astype(jnp.float32)
        middle = rest.astype(jnp.bfloat16)
        low = (rest - middle.astype(jnp.float32)).astype(jnp.bfloat16)
        dot = functools.partial(jnp.dot, preferred_element_type=jnp.float32)
        both = dot(times, jnp.concatenate([high, middle], axis=1))
        step = (dot(times, low) + both[:, width:]) + both[:, :width]
        partial[...] += step.reshape(partial.shape)
        return 0

    lax.fori_loop(0, block_len // depth, multiply, 0)

    low, high = lax.rem(r, half), lax.div(r, half)
    sum_copies = []
    for mr in range(1, half):
        pr, _ = peer(mr, 0)
        copy = pltpu.make_async_remote_copy(
            src_ref=partial.at[:, lax.rem(pr, half)], dst_ref=arrived.at[mr],
            send_sem=sum_send.at[mr], recv_sem=sum_recv.at[mr],
            device_id=(c, pr), device_id_type=MESH,
        )
        copy.start()
        sum_copies.append(copy)
    send(cuts[1], cuts[2])

    for copy in sum_copies:
        copy.wait()
    total = partial[:, low]
    for mr in range(1, half):
        total += arrived[mr]
    halves[...] = total
    own.wait()
    other, _ = peer(half, 0)
    across = pltpu.make_async_remote_copy(
        src_ref=halves.at[1 - high], dst_ref=crossed,
        send_sem=cross_send, recv_sem=cross_recv,
        device_id=(c, other), device_id_type=MESH,
    )
    across.start()
    send(cuts[2], len(order))
    across.wait()
    pooled_ref[...] = halves[high] + crossed[...]
    for copy in copies:
        copy.wait()


CUTS = (16, 21, 26)


def per_device(column_table, bag_rows):
    rows, cols = lax.axis_size("row"), lax.axis_size("col")
    block_len, width = column_table.shape
    own_bags, bag_len = bag_rows.shape
    span = block_len // (rows * cols)
    fits = (
        width % LANES == 0 and LANES % bag_len == 0 and own_bags * bag_len == SUBLANES * LANES
        and span % SUBLANES == 0 and block_len % LANES == 0
        and rows > 1 and rows & (rows - 1) == 0 and cols & (cols - 1) == 0
    )
    if not fits:
        return general(column_table, bag_rows)
    bags = own_bags * rows
    peers = rows * cols - 1
    half = rows // 2
    dma = pltpu.SemaphoreType.DMA
    landed, sums = pl.pallas_call(
        functools.partial(kernel, rows, cols),
        out_shape=(
            jax.ShapeDtypeStruct((rows, cols, span, width), jnp.float32),
            jax.ShapeDtypeStruct((own_bags, width), jnp.float32),
        ),
        in_specs=[pl.BlockSpec(memory_space=pltpu.HBM), pl.BlockSpec(memory_space=pltpu.HBM)],
        out_specs=(pl.BlockSpec(memory_space=pltpu.VMEM), pl.BlockSpec(memory_space=pltpu.VMEM)),
        scratch_shapes=[
            pltpu.VMEM((block_len, width), jnp.float32),
            pltpu.VMEM((own_bags, bag_len), jnp.int32),
            pltpu.VMEM((SUBLANES, LANES), jnp.int32),
            pltpu.VMEM((rows, SUBLANES, LANES), jnp.int32),
            pltpu.VMEM((bags, block_len), jnp.float32),
            pltpu.VMEM((2, half, own_bags, width), jnp.float32),
            pltpu.VMEM((half, 2, own_bags, width), jnp.float32),
            pltpu.VMEM((2, own_bags, width), jnp.float32),
            pltpu.VMEM((own_bags, width), jnp.float32),
            dma, dma, dma, dma((peers,)), dma((peers,)),
            dma((rows,)), dma((rows,)), dma((half,)), dma((half,)), dma, dma,
        ],
        compiler_params=pltpu.CompilerParams(
            collective_id=0, has_side_effects=True, vmem_limit_bytes=32 * 1024 * 1024
        ),
    )(
        pltpu.with_memory_space_constraint(column_table, pltpu.HBM),
        pltpu.with_memory_space_constraint(bag_rows, pltpu.HBM),
    )
    return pl.pallas_call(
        write_out,
        out_shape=(
            jax.ShapeDtypeStruct((rows, span, width * cols), jnp.float32),
            jax.ShapeDtypeStruct((own_bags, width), jnp.float32),
        ),
        in_specs=[pl.BlockSpec(memory_space=pltpu.VMEM)] * 2,
        out_specs=(pl.BlockSpec(memory_space=pltpu.HBM), pl.BlockSpec(memory_space=pltpu.HBM)),
        scratch_shapes=[dma((cols,)), dma],
        compiler_params=pltpu.CompilerParams(vmem_limit_bytes=8 * 1024 * 1024),
    )(landed, sums)


def write_out(landed_ref, sums_ref, out_ref, pooled_ref, sems, sum_sem):
    rows, cols, _, width = landed_ref.shape
    copies = [pltpu.make_async_copy(sums_ref, pooled_ref, sum_sem)]
    for c in range(cols):
        copies.append(pltpu.make_async_copy(
            landed_ref.at[:, c], out_ref.at[:, :, c * width:(c + 1) * width], sems.at[c]
        ))
    for copy in copies:
        copy.start()
    for copy in copies:
        copy.wait()


def solution(mesh):
    return jax.shard_map(
        per_device,
        mesh=mesh,
        in_specs=(P("row", "col"), P("row", None)),
        out_specs=(P(None, ("col", "row"), None), P("row", "col")),
        check_vma=False,
    )
```
